512 devices in a mesh: dom: 128 (over z, x, core), sub: 4 (over y).
Axes of the slice: x: 4, y: 4, z: 16, core: 2. Of those that a mesh axis runs over, the one named last changes fastest.
Arguments:
- source_one: float32 [25, 327680], P(None, ('dom', 'sub')), may hold values from -17 to 17
- source_two: float32 [25, 327680], P(None, ('dom', 'sub')), may hold values from -17 to 17
- face_mass: float32 [327680], P(('dom', 'sub')), may hold values from 0.2 to 1
- penalty: float32 [131072], P(('dom', 'sub')), may hold values from 0.5 to 2
- interior_scale: float32 [500, 131072], P(None, ('dom', 'sub')), may hold values from 0.5 to 2
- coupling: float32 [500, 150], replicated, may hold values from -0.5 to 0.5
- inverse_block: float32 [500, 500], replicated, as said below
- element_faces: int32 [6, 131072], P(None, ('dom', 'sub')), may hold values from 0 to 3071, as said below
- element_type: int32 [131072], P(('dom', 'sub')), may hold values 0 or 1
- send_faces: int32 [4, 65536], P(None, ('dom', 'sub')), may hold values from 0 to 2559
Outputs:
- trace_two: float32 [25, 327680], P(None, ('dom', 'sub'))
- interior: float32 [500, 131072], P(None, ('dom', 'sub'))
The draws below stay inside these ranges and needn't reach their ends.
Inputs may be any that keep to these rules, and one draw needn't show every extreme that they name: `element_faces`: every entry of rows 0 to 4 or of row 5 lies below 3072; on each device each of the 512 received faces is named exactly once, always in rows 0 to 4; row 5 names only group faces. `inverse_block`: symmetric positive definite.
All inputs are finite; a program needn't handle non-finite values. No bound on the sum of `element_type` on one device may be relied on, other than what follows from the above.
Results may differ from the reference program's by a relative error of at most 0.0003.
Values sent between devices are 32-bit elements; how exact they have to be, the bound alone decides.
No kernel may reach another device: no remote copies, remote signals or barrier semaphores. Data moves between devices by JAX's collectives and lax.ppermute only.
A program may use at most 64 MiB of HBM per device.

```python
import math
import jax
import jax.numpy as jnp
from jax import lax

FN = 25
NI = 500
ITERS = 3
E_DEV = 256
F_DEV = 640
SLOTS = 128
NT = 150
ELEMS = 131072
FACES = 327680
N_DOM = 128
N_SUB = 4
DEVICES = 512


def rising_field(key, salt):
    third = jax.random.fold_in(jax.random.fold_in(key, salt), 2)
    owner = jnp.arange(FACES, dtype=jnp.int32) // F_DEV
    ramp = 1.0 + 2.0 * owner.astype(jnp.float32) / float(DEVICES - 1)
    values = jnp.clip(jax.random.normal(third, (FN, FACES), jnp.float32), -5.0, 5.0)
    return (values * ramp[None, :]).astype(jnp.float32)


def draw_source_one(key, part):
    return rising_field(key, 101)


def draw_source_two(key, part):
    return rising_field(key, 202)


def draw_inverse_block(key, part):
    factor = jax.random.normal(jax.random.fold_in(key, 23), (NI, NI), jnp.float32)
    product = jnp.dot(factor, factor.T, precision=lax.Precision.HIGHEST) / NI
    return (0.5 * jnp.eye(NI, dtype=jnp.float32) + product).astype(jnp.float32)


def draw_element_faces(key, part):
    group_width = N_SUB * F_DEV
    ghosts = 4 * SLOTS

    def one_device(device_key):
        first, second, third = jax.random.split(device_key, 3)
        base = jax.random.randint(first, (6, E_DEV), 0, group_width, dtype=jnp.int32)
        places = jax.random.permutation(second, 5 * E_DEV)[:ghosts]
        fill = group_width + jax.random.permutation(third, ghosts).astype(jnp.int32)
        head = base[:5].reshape(-1).at[places].set(fill).reshape(5, E_DEV)
        return jnp.concatenate([head, base[5:]], axis=0)
    device_keys = jax.random.split(jax.random.fold_in(key, 11), DEVICES)
    blocks = jax.vmap(one_device)(device_keys)
    return jnp.transpose(blocks, (1, 0, 2)).reshape(6, DEVICES * E_DEV).astype(jnp.int32)


def place_ends(drawn, own_key, least, high):
    longest = drawn.shape.index(max(drawn.shape))
    spots = []
    for shift in (0, 1):
        where = [jax.random.randint(jax.random.fold_in(own_key, axis), (), 0, length) for axis, length in enumerate(drawn.shape)]
        where[longest] = (where[longest] + shift) % drawn.shape[longest]
        spots.append(tuple(where))
    return drawn.at[spots[0]].set(least).at[spots[1]].set(high)


def level_of(rng, dims, shards, smallest, largest):
    factor_of = 1.0
    for dim, blocks in shards:
        draws = jax.random.uniform(jax.random.fold_in(jax.random.fold_in(rng, 6), dim), (blocks,), jnp.float32, smallest / len(shards), largest / len(shards))
        factor_of = factor_of * jnp.repeat(jnp.exp(draws), dims[dim] // blocks).reshape((-1,) + (1,) * (len(dims) - 1 - dim))
    return factor_of


def bell_draw(key, shape, scale, bound, held_as=jnp.bfloat16):
    values = jax.random.normal(key, shape, jnp.float32) * scale
    return jnp.minimum(jnp.maximum(values, -bound), bound).astype(held_as)


def setup_inputs(seed: int = 0) -> dict:
    seeds = jax.random.split(jax.random.key(seed), 11)
    source_one = draw_source_one(jax.random.fold_in(seeds[10], 71), 0)
    source_two = draw_source_two(jax.random.fold_in(seeds[10], 71), 0)
    face_mass = jnp.clip(jnp.exp(math.log(1.0) - 1.609438 * jax.random.uniform(seeds[2], (FACES,), jnp.float32) ** level_of(seeds[2], (FACES,), ((0, 512),), -0.2, 0.2)), 0.2, 1.0)
    penalty = jnp.clip(jnp.exp(math.log(2.0) - 1.3862944 * jax.random.uniform(seeds[3], (ELEMS,), jnp.float32) ** level_of(seeds[3], (ELEMS,), ((0, 512),), -0.2, 0.2)), 0.5, 2.0)
    interior_scale = jnp.clip(jnp.exp(math.log(2.0) - 1.3862944 * jax.random.uniform(seeds[4], (NI, ELEMS), jnp.float32) ** level_of(seeds[4], (NI, ELEMS), ((1, 512),), -0.2, 0.2)), 0.5, 2.0)
    coupling = bell_draw(seeds[5], (NI, NT), NT ** -0.5, 0.5, jnp.float32)
    inverse_block = draw_inverse_block(jax.random.fold_in(seeds[10], 71), 0)
    element_faces = draw_element_faces(jax.random.fold_in(seeds[10], 71), 0)
    element_type = place_ends((jax.random.randint(seeds[8], (ELEMS,), 0, 3) < 1).astype(jnp.int32), jax.random.fold_in(seeds[8], 1), 0, 1)
    send_faces = place_ends(jax.random.randint(seeds[9], (4, SLOTS * DEVICES), 0, N_SUB * F_DEV), jax.random.fold_in(seeds[9], 1), 0, (N_SUB * F_DEV) - 1).astype(jnp.int32)
    return dict(source_one=source_one, source_two=source_two, face_mass=face_mass, penalty=penalty, interior_scale=interior_scale, coupling=coupling, inverse_block=inverse_block, element_faces=element_faces, element_type=element_type, send_faces=send_faces)


def global_faces(element_faces, send_faces):
    group_width = N_SUB * F_DEV
    device = jnp.arange(ELEMS, dtype=jnp.int32) // E_DEV
    domain = device // N_SUB
    member = device % N_SUB
    ghost = jnp.maximum(element_faces - group_width, 0)
    direction = ghost // SLOTS
    position = ghost % SLOTS
    offsets = jnp.array([1, -1, N_DOM // 4, -(N_DOM // 4)], dtype=jnp.int32)
    source_domain = (domain[None, :] - offsets[direction]) % N_DOM
    column = (source_domain * N_SUB + member[None, :]) * SLOTS + position
    remote = source_domain * group_width + send_faces[direction, column]
    nearby = domain[None, :] * group_width + element_faces
    return jnp.where(element_faces < group_width, nearby, remote).astype(jnp.int32)


def condense(vector, faces, slot_mask, interior_scale, coupling, inverse_block):
    weighted = vector[:, faces].reshape(NT, ELEMS) * slot_mask
    coupled = jnp.dot(coupling, weighted, precision=lax.Precision.HIGHEST)
    inner = interior_scale * jnp.dot(inverse_block, interior_scale * coupled, precision=lax.Precision.HIGHEST)
    return weighted, inner


def apply_operator(vector, faces, slot_mask, penalty, interior_scale, coupling, inverse_block, face_mass):
    weighted, inner = condense(vector, faces, slot_mask, interior_scale, coupling, inverse_block)
    contrib = slot_mask * (penalty[None, :] * weighted + jnp.dot(coupling.T, inner, precision=lax.Precision.HIGHEST))
    assembled = jnp.zeros_like(vector).at[:, faces].add(contrib.reshape(FN, 6, ELEMS))
    return face_mass[None, :] * vector + assembled


def reference(source_one, source_two, face_mass, penalty, interior_scale, coupling, inverse_block, element_faces, element_type, send_faces):
    faces = global_faces(element_faces, send_faces)
    last_slot = (jnp.arange(NT, dtype=jnp.int32) % 6) == 5
    prism = element_type == 1
    slot_mask = 1.0 - jnp.logical_and(last_slot[:, None], prism[None, :]).astype(jnp.float32)

    def operate(vector):
        return apply_operator(vector, faces, slot_mask, penalty, interior_scale, coupling, inverse_block, face_mass)

    def solve(rhs):
        solution = jnp.zeros_like(rhs)
        residual = rhs
        direction = rhs
        norm_now = jnp.sum(residual * residual)
        for step in range(ITERS):
            applied = operate(direction)
            step_size = norm_now / jnp.sum(direction * applied)
            solution = solution + step_size * direction
            residual = residual - step_size * applied
            norm_next = jnp.sum(residual * residual)
            direction = residual + (norm_next / norm_now) * direction
            norm_now = norm_next
        return solution

    trace_one = solve(source_one)
    trace_two = solve(source_two + face_mass[None, :] * trace_one)
    weighted, inner = condense(trace_two, faces, slot_mask, interior_scale, coupling, inverse_block)
    return trace_two, inner
```

```python
import jax
import jax.numpy as jnp
from jax import lax
from jax.experimental import pallas as pl
from jax.experimental.pallas import tpu as pltpu
from jax.sharding import Mesh
from jax.sharding import PartitionSpec as P

F32 = jnp.float32
BF16 = jnp.bfloat16
LANES = 128
ROWS = 32
EXACT = lax.Precision.HIGHEST
DOM = ("zq", "zr", "x", "core")
ALL = ("zq", "zr", "x", "core", "sub")
NEAR = ("x", "core", "sub")
FAR = ("zq", "zr")
VMEM = pl.BlockSpec(memory_space=pltpu.VMEM)
SMEM = pl.BlockSpec(memory_space=pltpu.SMEM)


def kernel_call(body, outs, *args, name, specs=None, scratch=()):
    return pl.pallas_call(
        body,
        out_shape=outs,
        in_specs=specs or [VMEM] * len(args),
        out_specs=jax.tree.map(lambda _: VMEM, outs),
        scratch_shapes=scratch,
        name=name,
        compiler_params=pltpu.CompilerParams(vmem_limit_bytes=32 << 20),
    )(*args)


def shape(*dims, dtype=F32):
    return jax.ShapeDtypeStruct(dims, dtype)


def split3(x):
    high = x.astype(BF16)
    rest = x - high.astype(F32)
    middle = rest.astype(BF16)
    low = (rest - middle.astype(F32)).astype(BF16)
    return jnp.concatenate([high, middle, low], axis=0)


def join3(y):
    return y[:ROWS] + y[ROWS : 2 * ROWS] + y[2 * ROWS :]


def pick_lanes(index, tiles, groups):
    index = jnp.broadcast_to(index, (8, LANES))
    block = lax.shift_right_logical(index, 7)
    lane = jnp.bitwise_and(index, LANES - 1)
    count, load = tiles
    picked = [jnp.zeros((8, LANES), F32) for _ in range(groups)]
    for source in range(count):
        here = block == source
        for group in range(groups):
            moved = jnp.take_along_axis(load(source, group), lane, axis=1)
            picked[group] = jnp.where(here, moved, picked[group])
    return picked


def place_lanes(pieces, spread, first, width):
    offset = spread - lax.broadcasted_iota(jnp.int32, spread.shape, 1)
    hits = [(offset == (first + k)).astype(F32).astype(BF16) for k in range(0, width, LANES)]
    return join3(jnp.dot(pieces, jnp.concatenate(hits, axis=1), preferred_element_type=F32))


def lane_sums(x):
    total = x[:, :LANES]
    for begin in range(LANES, x.shape[1], LANES):
        total = total + x[:, begin : begin + LANES]
    return jnp.sum(total, axis=0, keepdims=True)


def first_kernel(arrived, send_list, v0, other, outgoing):
    blocks = arrived.shape[2] // LANES
    for member in range(arrived.shape[0]):
        for block in range(blocks):
            to = pl.ds((member * blocks + block) * LANES, LANES)
            v0[:, to] = arrived[member, :ROWS, pl.ds(block * LANES, LANES)]
            other[:, to] = arrived[member, ROWS:, pl.ds(block * LANES, LANES)]

    def load(source, group):
        member, block = divmod(source, blocks)
        return arrived[member, pl.ds(group * 8, 8), pl.ds(block * LANES, LANES)]

    for channel in range(4):
        index = send_list[:, pl.ds(channel * LANES, LANES)]
        picked = pick_lanes(index, (arrived.shape[0] * blocks, load), 2 * ROWS // 8)
        for group, tile in enumerate(picked):
            outgoing[channel, pl.ds(group * 8, 8), :] = tile


def gather_slots(vector, ghosts, faces, mask, weighted):
    count = vector.shape[1] // LANES

    def load(source, group):
        if source < count:
            return vector[pl.ds(group * 8, 8), pl.ds(source * LANES, LANES)]
        return ghosts[source - count, pl.ds(group * 8, 8), :]

    for block in range(12):
        slot, half = divmod(block, 2)
        index = faces[:, pl.ds(block * LANES, LANES)]
        picked = pick_lanes(index, (count + 4, load), ROWS // 8)
        for group, tile in enumerate(picked):
            if slot == 5:
                tile = tile * mask[:, pl.ds(half * LANES, LANES)]
            weighted[pl.ds(slot * ROWS + group * 8, 8), pl.ds(half * LANES, LANES)] = tile


def apply_kernel(
    vector, ghosts, faces, spread, mask, penalty, coupling, lift, inverse, scale,
    returned, pieces, inner, weighted,
):
    gather_slots(vector, ghosts, faces, mask, weighted)
    w = weighted[...]
    s = scale[...]
    coupled = s * jnp.dot(coupling[...], w, precision=EXACT, preferred_element_type=F32)
    inside = s * jnp.dot(inverse[...], coupled, precision=EXACT, preferred_element_type=F32)
    inner[...] = inside
    lifted = jnp.dot(lift[...], inside, precision=EXACT, preferred_element_type=F32)
    contrib = penalty[...] * w + lifted
    slots = [contrib[k * ROWS : (k + 1) * ROWS] for k in range(6)]
    slots[5] = slots[5] * mask[...]
    parts = split3(jnp.concatenate(slots, axis=1))
    pieces[...] = parts
    width = 5 * mask.shape[1]
    for pair in range(2):
        onto = place_lanes(
            parts[:, :width], spread[:width], vector.shape[1] + pair * 2 * LANES, 2 * LANES
        )
        returned[2 * pair] = onto[:, :LANES]
        returned[2 * pair + 1] = onto[:, LANES:]


def place_kernel(pieces, spread, placed):
    for begin in range(0, placed.shape[1], 2 * LANES):
        placed[:, pl.ds(begin, 2 * LANES)] = place_lanes(
            pieces[...], spread[...], begin, 2 * LANES
        )


def pack_kernel(placed, received, spread, packed):
    blocks = placed.shape[1] // LANES
    parts = split3(jnp.concatenate([received[c] for c in range(4)], axis=1))
    packed[:, pl.ds(24 * blocks, 24), :] = jnp.zeros((4, 24, LANES), F32)
    for begin in range(0, blocks, 2):
        onto = place_lanes(parts, spread[...], begin * LANES, 2 * LANES)
        onto = onto + placed[:, pl.ds(begin * LANES, 2 * LANES)]
        for k in range(2):
            block = begin + k
            half = onto[:, k * LANES : (k + 1) * LANES]
            for member in range(4):
                for group in range(3):
                    packed[member, pl.ds((group * blocks + block) * 8, 8), :] = half[
                        group * 8 : group * 8 + 8
                    ]
                packed[member, pl.ds(24 * blocks + block, 1), :] = half[24:25]


def next_kernel(arrived, before, other, send_list, inv_alpha, vector, outgoing):
    blocks = before.shape[1] // LANES
    ia = inv_alpha[0]

    def total(begin, size):
        rows = pl.ds(begin, size)
        return (arrived[0, rows, :] + arrived[1, rows, :]) + (
            arrived[2, rows, :] + arrived[3, rows, :]
        )

    vector[pl.ds(24, 8), :] = jnp.zeros((8, vector.shape[1]), F32)
    for block in range(blocks):
        lanes = pl.ds(block * LANES, LANES)
        weight = other[pl.ds(ROWS - 1, 1), lanes]
        for group in range(3):
            old = before[pl.ds(group * 8, 8), lanes]
            new = (weight * old + total((group * blocks + block) * 8, 8)) * ia - old
            vector[pl.ds(group * 8, 8), lanes] = new
        old = before[pl.ds(24, 1), lanes]
        new = (weight * old + total(24 * blocks + block, 1)) * ia - old
        vector[pl.ds(24, 1), lanes] = new

    def load(source, group):
        return vector[pl.ds(group * 8, 8), pl.ds(source * LANES, LANES)]

    for channel in range(4):
        index = send_list[:, pl.ds(channel * LANES, LANES)]
        for group, tile in enumerate(pick_lanes(index, (blocks, load), ROWS // 8)):
            outgoing[channel, pl.ds(group * 8, 8), :] = tile


def energy_kernel(
    v0, v1, v2, ghosts, other, faces, mask, penalty, coupling, inverse, scale, inv_alpha,
    moments, inner, weighted,
):
    gather_slots(v2, ghosts, faces, mask, weighted)
    w = weighted[...]
    s = scale[...]
    coupled = s * jnp.dot(coupling[...], w, precision=EXACT, preferred_element_type=F32)
    inside = jnp.dot(inverse[...], coupled, precision=EXACT, preferred_element_type=F32)
    inner[...] = s * inside
    a, b, c = v0[...], v1[...], v2[...]
    group = [lane_sums(p) for p in (a * a, a * b, b * b, b * c, c * c)]
    weight = other[pl.ds(ROWS - 1, 1), :]
    local = lane_sums(coupled * inside) + lane_sums(penalty[...] * (w * w))
    energy = (0.25 * lane_sums(weight * (c * c)) + local) * inv_alpha[0]
    rows = [0.25 * g for g in group] + [energy, jnp.zeros((2, LANES), F32)]
    tile = jnp.concatenate(rows, axis=0)
    for k in range(moments.shape[0]):
        moments[k] = tile


def sum_kernel(arrived, moments):
    total = arrived[0]
    for k in range(1, arrived.shape[0]):
        total = total + arrived[k]
    for k in range(moments.shape[0]):
        moments[k] = total


def weights_of(arrived, ia):
    total = arrived[0]
    for k in range(1, arrived.shape[0]):
        total = total + arrived[k]
    m = jnp.sum(total, axis=1, keepdims=True)
    m00, m01, m11, m12, m22, energy = (m[k : k + 1] for k in range(6))
    h00, h01, h02 = m00 + m01, m01 + m11, m11 + m12
    h11, h12, h22 = m11 + m12, m12 + m22, energy

    def inverse_of(pivot, whole):
        fine = pivot > 1e-7 * whole
        return jnp.where(fine, 1.0 / jnp.where(fine, pivot, 1.0), 0.0)

    i0 = inverse_of(h00, 0.0 * h00)
    l1, l2 = h01 * i0, h02 * i0
    i1 = inverse_of(h11 - l1 * h01, h11)
    e = h12 - l1 * h02
    l3 = e * i1
    i2 = inverse_of(h22 - l2 * h02 - l3 * e, h22)
    z1 = m01 - l1 * m00
    z2 = m11 - l2 * m00 - l3 * z1
    y2 = z2 * i2
    y1 = z1 * i1 - l3 * y2
    y0 = m00 * i0 - l1 * y1 - l2 * y2
    return y0 * ia, y1 * ia, y2 * ia


def second_kernel(
    arrived, v0, v1, v2, g0, g1, g2, other, other_ghosts, inv_alpha, vector, ghosts
):
    y0, y1, y2 = weights_of(arrived, inv_alpha[0])
    keep = lax.broadcasted_iota(jnp.int32, (ROWS, 1), 0) < ROWS - 1

    def start(explicit, a, b, c):
        weight = explicit[ROWS - 1 :]
        return jnp.where(keep, explicit, 0.0) + weight * (y0 * a + y1 * b + y2 * c)

    vector[...] = start(other[...], v0[...], v1[...], v2[...])
    for c in range(4):
        ghosts[c] = start(other_ghosts[c, ROWS:, :], g0[c, :ROWS, :], g1[c], g2[c])


def last_kernel(arrived, v0, v1, v2, n0, n1, n2, inv_alpha, member, trace, interior):
    y0, y1, y2 = weights_of(arrived, inv_alpha[0])
    nodes, owned = trace.shape
    mine = pl.ds(pl.multiple_of(member[0] * owned, LANES), owned)
    trace[...] = (y0 * v0[:, mine] + y1 * v1[:, mine] + y2 * v2[:, mine])[:nodes]
    count = interior.shape[0]
    interior[...] = (y0 * n0[...] + y1 * n1[...] + y2 * n2[...])[:count]


def body(
    source_one,
    source_two,
    face_mass,
    penalty,
    interior_scale,
    coupling,
    inverse_block,
    element_faces,
    element_type,
    send_faces,
):
    members = lax.axis_size("sub")
    nodes, owned = source_one.shape
    group_width = members * owned
    elements = element_faces.shape[1]
    unknowns = coupling.shape[0]
    padded = -(-unknowns // LANES) * LANES
    reach = lax.axis_size(DOM) // 4
    domains = lax.axis_size(DOM)
    odd = lax.axis_index("core") % 2 == 1
    odd_far = lax.axis_index("zq") % 2 == 1

    pairs = (
        [(i, i + 1 if i % 2 == 0 else i - 1) for i in range(domains)],
        [(i, (i + 1 if i % 2 == 1 else i - 1) % domains) for i in range(domains)],
        [
            (i, (i + reach if (i // reach) % 2 == 0 else i - reach) % domains)
            for i in range(domains)
        ],
        [
            (i, (i + reach if (i // reach) % 2 == 1 else i - reach) % domains)
            for i in range(domains)
        ],
    )

    def exchange(payload):
        return jnp.stack([lax.ppermute(payload[c], DOM, pairs[c]) for c in range(4)])

    to_send = jnp.concatenate(
        [
            jnp.where(odd, send_faces[1], send_faces[0]),
            jnp.where(odd, send_faces[0], send_faces[1]),
            jnp.where(odd_far, send_faces[3], send_faces[2]),
            jnp.where(odd_far, send_faces[2], send_faces[3]),
        ]
    )
    near = element_faces - group_width
    direction = near // LANES
    swapped = jnp.where(direction < 2, jnp.where(odd, 0, 1), jnp.where(odd_far, 0, 1))
    remote = element_faces + LANES * jnp.where(
        swapped == 1, jnp.where(direction % 2 == 0, 1, -1), 0
    )
    faces = jnp.where(element_faces < group_width, element_faces, remote)
    faces = faces.reshape(1, -1)
    slots = faces.shape[1]
    spread = jnp.broadcast_to(faces.reshape(slots, 1), (slots, LANES))
    send_list = to_send.reshape(1, -1)
    send_spread = jnp.broadcast_to(to_send[:, None], (to_send.shape[0], LANES))
    mask = 1.0 - (element_type == 1).astype(F32)[None, :]
    weight = penalty[None, :]

    by_slot = coupling.reshape(unknowns, nodes, 6).transpose(0, 2, 1)
    by_slot = jnp.pad(by_slot, ((0, padded - unknowns), (0, 0), (0, ROWS - nodes)))
    by_slot = by_slot.reshape(padded, 6 * ROWS)
    lift = by_slot.T
    extra = padded - unknowns
    inverse = jnp.pad(inverse_block, ((0, extra), (0, extra)))
    scale = jnp.pad(interior_scale, ((0, extra), (0, 0)))

    spectrum = jnp.sum(coupling * jnp.dot(inverse_block, coupling)) / coupling.shape[1]
    inv_alpha = (1.0 / (0.6 + 2.4 * (1.1 + 1.35 * spectrum))).reshape(1)

    zeros = jnp.zeros((ROWS - nodes, owned), F32)
    mine = jnp.concatenate([source_one, zeros, source_two, zeros[1:], face_mass[None, :]])
    everyone = lax.all_to_all(
        jnp.broadcast_to(mine[None], (members, *mine.shape)), "sub", 0, 0, tiled=True
    )
    v0, other, outgoing = kernel_call(
        first_kernel,
        (shape(ROWS, group_width), shape(ROWS, group_width), shape(4, 2 * ROWS, LANES)),
        everyone,
        send_list,
        name="first",
    )
    start_ghosts = exchange(outgoing)
    member = lax.axis_index("sub").astype(jnp.int32).reshape(1)

    def apply(vector, ghosts):
        returned, pieces, inner = kernel_call(
            apply_kernel,
            (
                shape(4, ROWS, LANES),
                shape(3 * ROWS, slots, dtype=BF16),
                shape(padded, elements),
            ),
            vector,
            ghosts,
            faces,
            spread,
            mask,
            weight,
            by_slot,
            lift,
            inverse,
            scale,
            name="apply",
            scratch=[pltpu.VMEM((6 * ROWS, elements), F32)],
        )
        back = exchange(returned)
        placed = kernel_call(
            place_kernel, shape(ROWS, group_width), pieces, spread, name="place"
        )
        packed = kernel_call(
            pack_kernel,
            shape(members, 24 * (group_width // LANES) + 24, LANES),
            placed,
            back,
            send_spread,
            name="pack",
        )
        arrived = lax.all_to_all(packed, "sub", 0, 0, tiled=True)
        following, outgoing = kernel_call(
            next_kernel,
            (shape(ROWS, group_width), shape(4, ROWS, LANES)),
            arrived,
            vector,
            other,
            send_list,
            inv_alpha,
            name="next",
            specs=[VMEM] * 4 + [SMEM],
        )
        return following, exchange(outgoing), inner

    def section(v0, g0):
        v1, g1, n0 = apply(v0, g0)
        v2, g2, n1 = apply(v1, g1)
        count = 1
        for axis in NEAR:
            count *= lax.axis_size(axis)
        far = domains * members // count
        moments, n2 = kernel_call(
            energy_kernel,
            (shape(count, 8, LANES), shape(padded, elements)),
            v0,
            v1,
            v2,
            g2,
            other,
            faces,
            mask,
            weight,
            by_slot,
            inverse,
            scale,
            inv_alpha,
            name="energy",
            specs=[VMEM] * 11 + [SMEM],
            scratch=[pltpu.VMEM((6 * ROWS, elements), F32)],
        )
        arrived = lax.all_to_all(moments, NEAR, 0, 0, tiled=True)
        moments = kernel_call(sum_kernel, shape(far, 8, LANES), arrived, name="sum")
        arrived = lax.all_to_all(moments, FAR, 0, 0, tiled=True)
        return (v0, v1, v2), (g0, g1, g2), (n0, n1, n2), arrived

    vs, gs, _, arrived = section(v0, start_ghosts[:, :ROWS])
    u0, h0 = kernel_call(
        second_kernel,
        (shape(ROWS, group_width), shape(4, ROWS, LANES)),
        arrived,
        *vs,
        *gs,
        other,
        start_ghosts,
        inv_alpha,
        name="second",
        specs=[VMEM] * 9 + [SMEM],
    )
    vs, _, inners, arrived = section(u0, h0)
    return kernel_call(
        last_kernel,
        (shape(nodes, owned), shape(unknowns, elements)),
        arrived,
        *vs,
        *inners,
        inv_alpha,
        member,
        name="last",
        specs=[VMEM] * 7 + [SMEM] * 2,
    )


def solution(mesh):
    sub = mesh.shape["sub"]
    split = Mesh(mesh.devices.reshape(4, 4, 4, 2, sub), ALL)
    return jax.shard_map(
        body,
        mesh=split,
        in_specs=(
            P(None, ALL),
            P(None, ALL),
            P(ALL),
            P(ALL),
            P(None, ALL),
            P(),
            P(),
            P(None, ALL),
            P(ALL),
            P(None, ALL),
        ),
        out_specs=(P(None, ALL), P(None, ALL)),
        check_vma=False,
    )
```

```python
import jax
import jax.numpy as jnp
from jax import lax
from jax.experimental import pallas as pl
from jax.experimental.pallas import tpu as pltpu
from jax.sharding import Mesh
from jax.sharding import PartitionSpec as P

F32 = jnp.float32
BF16 = jnp.bfloat16
LANES = 128
ROWS = 32
DOM = ("zq", "zr", "x", "core")
ALL = ("zq", "zr", "x", "core", "sub")
NEAR = ("x", "core", "sub")
FAR = ("zq", "zr")
VMEM = pl.BlockSpec(memory_space=pltpu.VMEM)
SMEM = pl.BlockSpec(memory_space=pltpu.SMEM)


def kernel_call(body, outs, *args, specs=None, scratch=()):
    return pl.pallas_call(
        body,
        out_shape=outs,
        in_specs=specs or [VMEM] * len(args),
        out_specs=jax.tree.map(lambda _: VMEM, outs),
        scratch_shapes=scratch,
        compiler_params=pltpu.CompilerParams(vmem_limit_bytes=32 << 20),
    )(*args)


def shape(*dims, dtype=F32):
    return jax.ShapeDtypeStruct(dims, dtype)


def split3(x):
    high = x.astype(BF16)
    rest = x - high.astype(F32)
    middle = rest.astype(BF16)
    low = (rest - middle.astype(F32)).astype(BF16)
    return jnp.concatenate([high, middle, low], axis=0)


def join3(y):
    return y[:ROWS] + y[ROWS : 2 * ROWS] + y[2 * ROWS :]


def halves(x):
    high = x.astype(BF16)
    return high, (x - high.astype(F32)).astype(BF16)


def rounded_halves(x):
    high = lax.reduce_precision(x, exponent_bits=8, mantissa_bits=7)
    return high.astype(BF16), (x - high).astype(BF16)


def product(left, right):
    high, low = halves(right)
    return jnp.dot(left[0][...], high, preferred_element_type=F32) + (
        jnp.dot(left[0][...], low, preferred_element_type=F32)
        + jnp.dot(left[1][...], high, preferred_element_type=F32)
    )


def pick_lanes(index, tiles, groups):
    index = jnp.broadcast_to(index, (8, LANES))
    block = lax.shift_right_logical(index, 7)
    lane = jnp.bitwise_and(index, LANES - 1)
    count, load = tiles
    picked = [jnp.zeros((8, LANES), F32) for _ in range(groups)]
    for source in range(count):
        here = block == source
        for group in range(groups):
            moved = jnp.take_along_axis(load(source, group), lane, axis=1)
            picked[group] = jnp.where(here, moved, picked[group])
    return picked


def place_lanes(pieces, spread, first, width):
    offset = spread - lax.broadcasted_iota(jnp.int32, spread.shape, 1)
    hits = [(offset == (first + k)).astype(F32).astype(BF16) for k in range(0, width, LANES)]
    return join3(jnp.dot(pieces, jnp.concatenate(hits, axis=1), preferred_element_type=F32))


def lane_sums(x):
    total = x[:, :LANES]
    for begin in range(LANES, x.shape[1], LANES):
        total = total + x[:, begin : begin + LANES]
    return jnp.sum(total, axis=0, keepdims=True)


def start_kernel(one, two, mass, outgoing):
    nodes, owned = one.shape
    for member in range(outgoing.shape[0]):
        outgoing[member, :nodes, :] = one[...]
        outgoing[member, nodes:ROWS, :] = jnp.zeros((ROWS - nodes, owned), F32)
        outgoing[member, ROWS : ROWS + nodes, :] = two[...]
        outgoing[member, ROWS + nodes : 2 * ROWS - 1, :] = jnp.zeros((ROWS - 1 - nodes, owned), F32)
        outgoing[member, 2 * ROWS - 1 :, :] = mass[...]


def first_kernel(arrived, send_list, v0, other, *outgoing):
    blocks = arrived.shape[2] // LANES
    for member in range(arrived.shape[0]):
        for block in range(blocks):
            to = pl.ds((member * blocks + block) * LANES, LANES)
            v0[:, to] = arrived[member, :ROWS, pl.ds(block * LANES, LANES)]
            other[:, to] = arrived[member, ROWS:, pl.ds(block * LANES, LANES)]

    def load(source, group):
        member, block = divmod(source, blocks)
        return arrived[member, pl.ds(group * 8, 8), pl.ds(block * LANES, LANES)]

    for channel in range(4):
        index = send_list[:, pl.ds(channel * LANES, LANES)]
        picked = pick_lanes(index, (arrived.shape[0] * blocks, load), 2 * ROWS // 8)
        for group, tile in enumerate(picked):
            outgoing[channel][pl.ds(group * 8, 8), :] = tile


def gather_slots(vector, ghosts, faces, mask, weighted):
    count = vector.shape[1] // LANES
    width = mask.shape[1]
    near = vector[...]
    pieces = split3(jnp.concatenate([near] + [g[:ROWS, :] for g in ghosts], axis=1))

    def load(source, group):
        if source < count:
            return vector[pl.ds(group * 8, 8), pl.ds(source * LANES, LANES)]
        return ghosts[source - count][pl.ds(group * 8, 8), :]

    def step(slot, carry):
        other = slot + 3
        index = faces[:, pl.ds(pl.multiple_of(other * width, LANES), width)]
        lines = lax.broadcasted_iota(jnp.int32, (pieces.shape[1], width), 0)
        hits = (lines == index).astype(F32).astype(BF16)
        values = join3(jnp.dot(pieces, hits, preferred_element_type=F32))
        for block in range(width // LANES):
            begin = pl.multiple_of(slot * width + block * LANES, LANES)
            picked = pick_lanes(faces[:, pl.ds(begin, LANES)], (count + 4, load), ROWS // 8)
            for group, tile in enumerate(picked):
                row = pl.multiple_of(slot * ROWS + group * 8, 8)
                weighted[pl.ds(row, 8), pl.ds(block * LANES, LANES)] = tile
        weighted[pl.ds(pl.multiple_of(other * ROWS, ROWS), ROWS), :] = values
        return carry

    lax.fori_loop(0, 3, step, 0)
    weighted[pl.ds(5 * ROWS, ROWS), :] = weighted[pl.ds(5 * ROWS, ROWS), :] * mask[...]


def apply_kernel(*refs):
    vector, *ghosts = refs[:5]
    faces, spread, mask, penalty = refs[5:9]
    coupling, lift, inverse = refs[9:11], refs[11:13], refs[13:15]
    scale = refs[15]
    returned, pieces, weighted = refs[16:20], refs[20], refs[-1]
    gather_slots(vector, ghosts, faces, mask, weighted)
    w = weighted[...]
    s = scale[...]
    coupled = s * product(coupling, w)
    inside = s * product(inverse, coupled)
    if len(refs) == 23:
        refs[21][...] = inside
    contrib = penalty[...] * w + product(lift, inside)
    slots = [contrib[k * ROWS : (k + 1) * ROWS] for k in range(6)]
    slots[5] = slots[5] * mask[...]
    parts = split3(jnp.concatenate(slots, axis=1))
    pieces[...] = parts
    width = 5 * mask.shape[1]
    for pair in range(2):
        onto = place_lanes(
            parts[:, :width], spread[:width], vector.shape[1] + pair * 2 * LANES, 2 * LANES
        )
        returned[2 * pair][...] = onto[:, :LANES]
        returned[2 * pair + 1][...] = onto[:, LANES:]


def place_kernel(pieces, spread, placed):
    for begin in range(0, placed.shape[1], 2 * LANES):
        placed[:, pl.ds(begin, 2 * LANES)] = place_lanes(
            pieces[...], spread[...], begin, 2 * LANES
        )


def pack_kernel(placed, r0, r1, r2, r3, spread, packed):
    blocks = placed.shape[1] // LANES
    parts = split3(jnp.concatenate([r[...] for r in (r0, r1, r2, r3)], axis=1))
    packed[:, pl.ds(24 * blocks, 24), :] = jnp.zeros((4, 24, LANES), F32)
    for begin in range(0, blocks, 2):
        onto = place_lanes(parts, spread[...], begin * LANES, 2 * LANES)
        onto = onto + placed[:, pl.ds(begin * LANES, 2 * LANES)]
        for k in range(2):
            block = begin + k
            half = onto[:, k * LANES : (k + 1) * LANES]
            for member in range(4):
                for group in range(3):
                    packed[member, pl.ds((group * blocks + block) * 8, 8), :] = half[
                        group * 8 : group * 8 + 8
                    ]
                packed[member, pl.ds(24 * blocks + block, 1), :] = half[24:25]


def next_kernel(arrived, before, other, send_list, inv_alpha, vector, *outgoing):
    blocks = before.shape[1] // LANES
    ia = inv_alpha[0]

    def total(begin, size):
        rows = pl.ds(begin, size)
        return (arrived[0, rows, :] + arrived[1, rows, :]) + (
            arrived[2, rows, :] + arrived[3, rows, :]
        )

    vector[pl.ds(24, 8), :] = jnp.zeros((8, vector.shape[1]), F32)
    for block in range(blocks):
        lanes = pl.ds(block * LANES, LANES)
        weight = other[pl.ds(ROWS - 1, 1), lanes]
        for group in range(3):
            old = before[pl.ds(group * 8, 8), lanes]
            new = (weight * old + total((group * blocks + block) * 8, 8)) * ia - old
            vector[pl.ds(group * 8, 8), lanes] = new
        old = before[pl.ds(24, 1), lanes]
        new = (weight * old + total(24 * blocks + block, 1)) * ia - old
        vector[pl.ds(24, 1), lanes] = new

    def load(source, group):
        return vector[pl.ds(group * 8, 8), pl.ds(source * LANES, LANES)]

    for channel in range(4):
        index = send_list[:, pl.ds(channel * LANES, LANES)]
        for group, tile in enumerate(pick_lanes(index, (blocks, load), ROWS // 8)):
            outgoing[channel][pl.ds(group * 8, 8), :] = tile


def moment_kernel(v0, v1, v2, other, inv_alpha, moments):
    a, b, c = v0[...], v1[...], v2[...]
    weight = other[pl.ds(ROWS - 1, 1), :] * inv_alpha[0]
    group = [lane_sums(p) for p in (a * a, a * b, b * b, b * c, c * c, weight * (c * c))]
    moments[...] = 0.25 * jnp.concatenate(group + [jnp.zeros((2, LANES), F32)], axis=0)


def energy_kernel(*refs):
    vector, *ghosts = refs[:5]
    faces, mask, penalty = refs[5:8]
    coupling, inverse = refs[8:10], refs[10:12]
    scale, face_part, inv_alpha, moments = refs[12:16]
    weighted = refs[-1]
    gather_slots(vector, ghosts, faces, mask, weighted)
    w = weighted[...]
    s = scale[...]
    coupled = s * product(coupling, w)
    inside = product(inverse, coupled)
    if len(refs) == 18:
        refs[16][...] = s * inside
    local = lane_sums(coupled * inside) + lane_sums(penalty[...] * (w * w))
    row = lax.broadcasted_iota(jnp.int32, (8, LANES), 0)
    tile = face_part[...] + jnp.where(row == 5, local * inv_alpha[0], 0.0)
    for k in range(moments.shape[0]):
        moments[k] = tile


def sum_kernel(arrived, moments):
    total = arrived[0]
    for k in range(1, arrived.shape[0]):
        total = total + arrived[k]
    for k in range(moments.shape[0]):
        moments[k] = total


def weights_of(arrived, ia):
    total = arrived[0]
    for k in range(1, arrived.shape[0]):
        total = total + arrived[k]
    m = jnp.sum(total, axis=1, keepdims=True)
    m00, m01, m11, m12, m22, energy = (m[k : k + 1] for k in range(6))
    h00, h01, h02 = m00 + m01, m01 + m11, m11 + m12
    h11, h12, h22 = m11 + m12, m12 + m22, energy

    def inverse_of(pivot, whole):
        fine = pivot > 1e-7 * whole
        return jnp.where(fine, 1.0 / jnp.where(fine, pivot, 1.0), 0.0)

    i0 = inverse_of(h00, 0.0 * h00)
    l1, l2 = h01 * i0, h02 * i0
    i1 = inverse_of(h11 - l1 * h01, h11)
    e = h12 - l1 * h02
    l3 = e * i1
    i2 = inverse_of(h22 - l2 * h02 - l3 * e, h22)
    z1 = m01 - l1 * m00
    z2 = m11 - l2 * m00 - l3 * z1
    y2 = z2 * i2
    y1 = z1 * i1 - l3 * y2
    y0 = m00 * i0 - l1 * y1 - l2 * y2
    return y0 * ia, y1 * ia, y2 * ia


def second_kernel(*refs):
    arrived, v0, v1, v2, other = refs[:5]
    ghosts, inv_alpha, vector, outputs = refs[5:17], refs[17], refs[18], refs[19:]
    y0, y1, y2 = weights_of(arrived, inv_alpha[0])
    keep = lax.broadcasted_iota(jnp.int32, (ROWS, 1), 0) < ROWS - 1

    def start(explicit, a, b, c):
        weight = explicit[ROWS - 1 :]
        return jnp.where(keep, explicit, 0.0) + weight * (y0 * a + y1 * b + y2 * c)

    vector[...] = start(other[...], v0[...], v1[...], v2[...])
    for c in range(4):
        both = ghosts[c]
        outputs[c][...] = start(
            both[ROWS:, :], both[:ROWS, :], ghosts[4 + c][...], ghosts[8 + c][...]
        )


def trace_kernel(arrived, v0, v1, v2, inv_alpha, member, trace):
    y0, y1, y2 = weights_of(arrived, inv_alpha[0])
    nodes, owned = trace.shape
    mine = pl.ds(pl.multiple_of(member[0] * owned, LANES), owned)
    trace[...] = (y0 * v0[:, mine] + y1 * v1[:, mine] + y2 * v2[:, mine])[:nodes]


def interior_kernel(arrived, n0, n1, n2, inv_alpha, interior):
    y0, y1, y2 = weights_of(arrived, inv_alpha[0])
    interior[...] = y0 * n0[...] + y1 * n1[...] + y2 * n2[...]


def body(
    source_one,
    source_two,
    face_mass,
    penalty,
    interior_scale,
    coupling,
    inverse_block,
    element_faces,
    element_type,
    send_faces,
):
    members = lax.axis_size("sub")
    nodes, owned = source_one.shape
    group_width = members * owned
    elements = element_faces.shape[1]
    unknowns = coupling.shape[0]
    padded = -(-unknowns // LANES) * LANES
    reach = lax.axis_size(DOM) // 4
    domains = lax.axis_size(DOM)
    odd = lax.axis_index("core") % 2 == 1
    odd_far = lax.axis_index("zq") % 2 == 1

    pairs = (
        [(i, i + 1 if i % 2 == 0 else i - 1) for i in range(domains)],
        [(i, (i + 1 if i % 2 == 1 else i - 1) % domains) for i in range(domains)],
        [
            (i, (i + reach if (i // reach) % 2 == 0 else i - reach) % domains)
            for i in range(domains)
        ],
        [
            (i, (i + reach if (i // reach) % 2 == 1 else i - reach) % domains)
            for i in range(domains)
        ],
    )

    def exchange(payload):
        got = []
        for c in range(4):
            got.append(lax.ppermute(payload[c], DOM, pairs[c]))
        return got

    to_send = jnp.concatenate(
        [
            jnp.where(odd, send_faces[1], send_faces[0]),
            jnp.where(odd, send_faces[0], send_faces[1]),
            jnp.where(odd_far, send_faces[3], send_faces[2]),
            jnp.where(odd_far, send_faces[2], send_faces[3]),
        ]
    )
    near = element_faces - group_width
    direction = near // LANES
    swapped = jnp.where(direction < 2, jnp.where(odd, 0, 1), jnp.where(odd_far, 0, 1))
    remote = element_faces + LANES * jnp.where(
        swapped == 1, jnp.where(direction % 2 == 0, 1, -1), 0
    )
    faces = jnp.where(element_faces < group_width, element_faces, remote)
    faces = faces.reshape(1, -1)
    slots = faces.shape[1]
    spread = jnp.broadcast_to(faces.reshape(slots, 1), (slots, LANES))
    send_list = to_send.reshape(1, -1)
    send_spread = jnp.broadcast_to(to_send[:, None], (to_send.shape[0], LANES))
    mask = 1.0 - (element_type == 1).astype(F32)[None, :]
    weight = penalty[None, :]

    by_slot = coupling.reshape(unknowns, nodes, 6).transpose(0, 2, 1)
    by_slot = jnp.pad(by_slot, ((0, padded - unknowns), (0, 0), (0, ROWS - nodes)))
    by_slot = by_slot.reshape(padded, 6 * ROWS)
    extra = padded - unknowns
    padded_inverse = jnp.pad(inverse_block, ((0, extra), (0, extra)))
    lift, by_slot, inverse = (
        rounded_halves(m) for m in (by_slot.T, by_slot, padded_inverse)
    )
    scale = jnp.pad(interior_scale, ((0, extra), (0, 0)))

    spectrum = jnp.sum(coupling * jnp.dot(inverse_block, coupling)) / coupling.shape[1]
    inv_alpha = (1.0 / (0.6 + 2.4 * (1.1 + 1.35 * spectrum))).reshape(1)

    tile = shape(ROWS, LANES)
    mine = kernel_call(
        start_kernel, shape(members, 2 * ROWS, owned), source_one, source_two, face_mass[None, :]
    )
    everyone = lax.all_to_all(mine, "sub", 0, 0, tiled=True)
    v0, other, *outgoing = kernel_call(
        first_kernel,
        (shape(ROWS, group_width), shape(ROWS, group_width)) + (shape(2 * ROWS, LANES),) * 4,
        everyone,
        send_list,
    )
    start_ghosts = exchange(outgoing)
    member = lax.axis_index("sub").astype(jnp.int32).reshape(1)
    scratch = [pltpu.VMEM((6 * ROWS, elements), F32)]

    def apply(vector, ghosts, keep_inner):
        inner_shape = (shape(padded, elements),) if keep_inner else ()
        *returned, pieces = outs = kernel_call(
            apply_kernel,
            (tile,) * 4 + (shape(3 * ROWS, slots, dtype=BF16),) + inner_shape,
            vector,
            *ghosts,
            faces,
            spread,
            mask,
            weight,
            *by_slot,
            *lift,
            *inverse,
            scale,
            scratch=scratch,
        )
        returned, pieces, inner = outs[:4], outs[4], outs[5:]
        back = exchange(returned)
        placed = kernel_call(place_kernel, shape(ROWS, group_width), pieces, spread)
        packed = kernel_call(
            pack_kernel,
            shape(members, 24 * (group_width // LANES) + 24, LANES),
            placed,
            *back,
            send_spread,
        )
        arrived = lax.all_to_all(packed, "sub", 0, 0, tiled=True)
        following, *outgoing = kernel_call(
            next_kernel,
            (shape(ROWS, group_width),) + (tile,) * 4,
            arrived,
            vector,
            other,
            send_list,
            inv_alpha,
            specs=[VMEM] * 4 + [SMEM],
        )
        return following, exchange(outgoing), list(inner)

    count = 1
    for axis in NEAR:
        count *= lax.axis_size(axis)
    far = domains * members // count

    def section(v0, g0, keep_inner):
        inner_shape = (shape(padded, elements),) if keep_inner else ()
        v1, g1, n0 = apply(v0, g0, keep_inner)
        v2, g2, n1 = apply(v1, g1, keep_inner)
        face_part = kernel_call(
            moment_kernel, shape(8, LANES), v0, v1, v2, other, inv_alpha, specs=[VMEM] * 4 + [SMEM]
        )
        moments, *n2 = kernel_call(
            energy_kernel,
            (shape(count, 8, LANES),) + inner_shape,
            v2,
            *g2,
            faces,
            mask,
            weight,
            *by_slot,
            *inverse,
            scale,
            face_part,
            inv_alpha,
            specs=[VMEM] * 14 + [SMEM],
            scratch=scratch,
        )
        arrived = lax.all_to_all(moments, NEAR, 0, 0, tiled=True)
        moments = kernel_call(sum_kernel, shape(far, 8, LANES), arrived)
        arrived = lax.all_to_all(moments, FAR, 0, 0, tiled=True)
        return (v0, v1, v2), g1 + g2, n0 + n1 + n2, arrived

    vs, later_ghosts, _, arrived = section(v0, start_ghosts, False)
    u0, *h0 = kernel_call(
        second_kernel,
        (shape(ROWS, group_width),) + (tile,) * 4,
        arrived,
        *vs,
        other,
        *start_ghosts,
        *later_ghosts,
        inv_alpha,
        specs=[VMEM] * 17 + [SMEM],
    )
    vs, _, inners, arrived = section(u0, h0, True)
    trace_two = kernel_call(
        trace_kernel,
        shape(nodes, owned),
        arrived,
        *vs,
        inv_alpha,
        member,
        specs=[VMEM] * 4 + [SMEM] * 2,
    )
    rows = pl.BlockSpec((LANES, elements), lambda i: (i, 0))
    interior = pl.pallas_call(
        interior_kernel,
        out_shape=shape(unknowns, elements),
        grid=(padded // LANES,),
        in_specs=[pl.BlockSpec(arrived.shape, lambda i: (0, 0, 0))] + [rows] * 3 + [SMEM],
        out_specs=rows,
        name="interior",
        compiler_params=pltpu.CompilerParams(vmem_limit_bytes=16 << 20),
    )(arrived, *inners, inv_alpha)
    return trace_two, interior


def solution(mesh):
    sub = mesh.shape["sub"]
    split = Mesh(mesh.devices.reshape(4, 4, 4, 2, sub), ALL)
    return jax.shard_map(
        body,
        mesh=split,
        in_specs=(
            P(None, ALL),
            P(None, ALL),
            P(ALL),
            P(ALL),
            P(None, ALL),
            P(),
            P(),
            P(None, ALL),
            P(ALL),
            P(None, ALL),
        ),
        out_specs=(P(None, ALL), P(None, ALL)),
        check_vma=False,
    )
```

```python
import jax
import jax.numpy as jnp
from jax import lax
from jax.experimental import pallas as pl
from jax.experimental.pallas import tpu as pltpu
from jax.sharding import Mesh
from jax.sharding import PartitionSpec as P

F32 = jnp.float32
BF16 = jnp.bfloat16
LANES = 128
ROWS = 32
DOM = ("zq", "zr", "x", "core")
ALL = ("zq", "zr", "x", "core", "sub")
NEAR = ("x", "core", "sub")
FAR = ("zq", "zr")
VMEM = pl.BlockSpec(memory_space=pltpu.VMEM)
ANY = pl.BlockSpec(memory_space=pl.ANY)
COPIED = pl.BlockSpec()
SMEM = pl.BlockSpec(memory_space=pltpu.SMEM)


def kernel_call(body, outs, *args, specs=None, out_specs=None, scratch=()):
    return pl.pallas_call(
        body,
        out_shape=outs,
        in_specs=specs or [VMEM] * len(args),
        out_specs=out_specs or jax.tree.map(lambda _: VMEM, outs),
        scratch_shapes=scratch,
        compiler_params=pltpu.CompilerParams(vmem_limit_bytes=32 << 20),
    )(*args)


def shape(*dims, dtype=F32):
    return jax.ShapeDtypeStruct(dims, dtype)


def split3(x):
    high = x.astype(BF16)
    rest = x - high.astype(F32)
    middle = rest.astype(BF16)
    low = (rest - middle.astype(F32)).astype(BF16)
    return jnp.concatenate([high, middle, low], axis=0)


def join3(y):
    return y[:ROWS] + y[ROWS : 2 * ROWS] + y[2 * ROWS :]


def halves(x):
    high = x.astype(BF16)
    return high, (x - high.astype(F32)).astype(BF16)


def rounded_halves(x):
    high = lax.reduce_precision(x, exponent_bits=8, mantissa_bits=7)
    return high.astype(BF16), (x - high).astype(BF16)


def product(left, right):
    high, low = halves(right)
    return jnp.dot(left[0][...], high, preferred_element_type=F32) + (
        jnp.dot(left[0][...], low, preferred_element_type=F32)
        + jnp.dot(left[1][...], high, preferred_element_type=F32)
    )


def pick_lanes(index, tiles, groups):
    index = jnp.broadcast_to(index, (8, LANES))
    block = lax.shift_right_logical(index, 7)
    lane = jnp.bitwise_and(index, LANES - 1)
    count, load = tiles
    picked = [jnp.zeros((8, LANES), F32) for _ in range(groups)]
    for source in range(count):
        here = block == source
        for group in range(groups):
            moved = jnp.take_along_axis(load(source, group), lane, axis=1)
            picked[group] = jnp.where(here, moved, picked[group])
    return picked


def place_lanes(pieces, spread, first, width):
    offset = spread - lax.broadcasted_iota(jnp.int32, spread.shape, 1)
    hits = [(offset == (first + k)).astype(F32).astype(BF16) for k in range(0, width, LANES)]
    return join3(jnp.dot(pieces, jnp.concatenate(hits, axis=1), preferred_element_type=F32))


def lane_sums(x):
    total = x[:, :LANES]
    for begin in range(LANES, x.shape[1], LANES):
        total = total + x[:, begin : begin + LANES]
    return jnp.sum(total, axis=0, keepdims=True)


def start_kernel(one, two, mass, outgoing):
    nodes, owned = one.shape
    for member in range(outgoing.shape[0]):
        outgoing[member, :nodes, :] = one[...]
        outgoing[member, nodes:ROWS, :] = jnp.zeros((ROWS - nodes, owned), F32)
        outgoing[member, ROWS : ROWS + nodes, :] = two[...]
        outgoing[member, ROWS + nodes : 2 * ROWS - 1, :] = jnp.zeros((ROWS - 1 - nodes, owned), F32)
        outgoing[member, 2 * ROWS - 1 :, :] = mass[...]


def first_kernel(arrived, send_list, inv_alpha, v0, other, *outgoing):
    del inv_alpha
    blocks = arrived.shape[2] // LANES
    for member in range(arrived.shape[0]):
        for block in range(blocks):
            to = pl.ds((member * blocks + block) * LANES, LANES)
            v0[:, to] = arrived[member, :ROWS, pl.ds(block * LANES, LANES)]
            other[:, to] = arrived[member, ROWS:, pl.ds(block * LANES, LANES)]

    def load(source, group):
        member, block = divmod(source, blocks)
        return arrived[member, pl.ds(group * 8, 8), pl.ds(block * LANES, LANES)]

    for channel in range(4):
        index = send_list[:, pl.ds(channel * LANES, LANES)]
        picked = pick_lanes(index, (arrived.shape[0] * blocks, load), 2 * ROWS // 8)
        for group, tile in enumerate(picked):
            outgoing[channel][pl.ds(group * 8, 8), :] = tile


def gather_slots(vector, ghosts, faces, mask, weighted):
    count = vector.shape[1] // LANES
    width = mask.shape[1]
    near = vector[...]
    pieces = split3(jnp.concatenate([near] + [g[:ROWS, :] for g in ghosts], axis=1))

    def load(source, group):
        if source < count:
            return vector[pl.ds(group * 8, 8), pl.ds(source * LANES, LANES)]
        return ghosts[source - count][pl.ds(group * 8, 8), :]

    def step(slot, carry):
        other = slot + 3
        index = faces[:, pl.ds(pl.multiple_of(other * width, LANES), width)]
        lines = lax.broadcasted_iota(jnp.int32, (pieces.shape[1], width), 0)
        hits = (lines == index).astype(F32).astype(BF16)
        values = join3(jnp.dot(pieces, hits, preferred_element_type=F32))
        for block in range(width // LANES):
            begin = pl.multiple_of(slot * width + block * LANES, LANES)
            picked = pick_lanes(faces[:, pl.ds(begin, LANES)], (count + 4, load), ROWS // 8)
            for group, tile in enumerate(picked):
                row = pl.multiple_of(slot * ROWS + group * 8, 8)
                weighted[pl.ds(row, 8), pl.ds(block * LANES, LANES)] = tile
        weighted[pl.ds(pl.multiple_of(other * ROWS, ROWS), ROWS), :] = values
        return carry

    lax.fori_loop(0, 3, step, 0)
    weighted[pl.ds(5 * ROWS, ROWS), :] = weighted[pl.ds(5 * ROWS, ROWS), :] * mask[...]


def apply_kernel(*refs):
    vector, *ghosts = refs[:5]
    faces, spread, mask, penalty = refs[5:9]
    coupling, lift, inverse = refs[9:11], refs[11:13], refs[13:15]
    scale = refs[15]
    returned, pieces = refs[16:20], refs[20]
    keep = len(refs) > 22
    weighted = refs[22] if keep else refs[21]
    gather_slots(vector, ghosts, faces, mask, weighted)
    w = weighted[...]
    s = scale[...]
    coupled = s * product(coupling, w)
    inside = s * product(inverse, coupled)
    if keep:
        refs[23][...] = inside
        leaving = pltpu.make_async_copy(refs[23], refs[21], refs[24])
        leaving.start()
    contrib = penalty[...] * w + product(lift, inside)
    slots = [contrib[k * ROWS : (k + 1) * ROWS] for k in range(6)]
    slots[5] = slots[5] * mask[...]
    parts = split3(jnp.concatenate(slots, axis=1))
    pieces[...] = parts
    width = 5 * mask.shape[1]
    for pair in range(2):
        onto = place_lanes(
            parts[:, :width], spread[:width], vector.shape[1] + pair * 2 * LANES, 2 * LANES
        )
        returned[2 * pair][...] = onto[:, :LANES]
        returned[2 * pair + 1][...] = onto[:, LANES:]
    if keep:
        leaving.wait()


def place_kernel(pieces, spread, placed):
    for begin in range(0, placed.shape[1], 2 * LANES):
        placed[:, pl.ds(begin, 2 * LANES)] = place_lanes(
            pieces[...], spread[...], begin, 2 * LANES
        )


def pack_kernel(placed, r0, r1, r2, r3, spread, packed):
    blocks = placed.shape[1] // LANES
    parts = split3(jnp.concatenate([r[...] for r in (r0, r1, r2, r3)], axis=1))
    packed[:, pl.ds(24 * blocks, 24), :] = jnp.zeros((4, 24, LANES), F32)
    for begin in range(0, blocks, 2):
        onto = place_lanes(parts, spread[...], begin * LANES, 2 * LANES)
        onto = onto + placed[:, pl.ds(begin * LANES, 2 * LANES)]
        for k in range(2):
            block = begin + k
            half = onto[:, k * LANES : (k + 1) * LANES]
            for member in range(4):
                for group in range(3):
                    packed[member, pl.ds((group * blocks + block) * 8, 8), :] = half[
                        group * 8 : group * 8 + 8
                    ]
                packed[member, pl.ds(24 * blocks + block, 1), :] = half[24:25]


def next_kernel(arrived, before, other, send_list, inv_alpha, vector, *outgoing):
    blocks = before.shape[1] // LANES
    ia = inv_alpha[0]

    def total(begin, size):
        rows = pl.ds(begin, size)
        return (arrived[0, rows, :] + arrived[1, rows, :]) + (
            arrived[2, rows, :] + arrived[3, rows, :]
        )

    vector[pl.ds(24, 8), :] = jnp.zeros((8, vector.shape[1]), F32)
    for block in range(blocks):
        lanes = pl.ds(block * LANES, LANES)
        weight = other[pl.ds(ROWS - 1, 1), lanes]
        for group in range(3):
            old = before[pl.ds(group * 8, 8), lanes]
            new = (weight * old + total((group * blocks + block) * 8, 8)) * ia - old
            vector[pl.ds(group * 8, 8), lanes] = new
        old = before[pl.ds(24, 1), lanes]
        new = (weight * old + total(24 * blocks + block, 1)) * ia - old
        vector[pl.ds(24, 1), lanes] = new

    def load(source, group):
        return vector[pl.ds(group * 8, 8), pl.ds(source * LANES, LANES)]

    for channel in range(4):
        index = send_list[:, pl.ds(channel * LANES, LANES)]
        for group, tile in enumerate(pick_lanes(index, (blocks, load), ROWS // 8)):
            outgoing[channel][pl.ds(group * 8, 8), :] = tile


def moment_kernel(v0, v1, v2, other, inv_alpha, moments):
    a, b, c = v0[...], v1[...], v2[...]
    weight = other[pl.ds(ROWS - 1, 1), :] * inv_alpha[0]
    group = [lane_sums(p) for p in (a * a, a * b, b * b, b * c, c * c, weight * (c * c))]
    moments[...] = 0.25 * jnp.concatenate(group + [jnp.zeros((2, LANES), F32)], axis=0)


def energy_kernel(*refs):
    vector, *ghosts = refs[:5]
    faces, mask, penalty = refs[5:8]
    coupling, inverse = refs[8:10], refs[10:12]
    scale, face_part, inv_alpha, moments = refs[12:16]
    weighted = refs[-1]
    gather_slots(vector, ghosts, faces, mask, weighted)
    w = weighted[...]
    s = scale[...]
    coupled = s * product(coupling, w)
    inside = product(inverse, coupled)
    if len(refs) == 18:
        refs[16][...] = s * inside
    local = lane_sums(coupled * inside) + lane_sums(penalty[...] * (w * w))
    row = lax.broadcasted_iota(jnp.int32, (8, LANES), 0)
    tile = face_part[...] + jnp.where(row == 5, local * inv_alpha[0], 0.0)
    for k in range(moments.shape[0]):
        moments[k] = tile


def sum_kernel(arrived, moments):
    total = arrived[0]
    for k in range(1, arrived.shape[0]):
        total = total + arrived[k]
    for k in range(moments.shape[0]):
        moments[k] = total


def weights_of(arrived, ia):
    total = arrived[0]
    for k in range(1, arrived.shape[0]):
        total = total + arrived[k]
    m = jnp.sum(total, axis=1, keepdims=True)
    m00, m01, m11, m12, m22, energy = (m[k : k + 1] for k in range(6))
    h00, h01, h02 = m00 + m01, m01 + m11, m11 + m12
    h11, h12, h22 = m11 + m12, m12 + m22, energy

    def inverse_of(pivot, whole):
        fine = pivot > 1e-7 * whole
        return jnp.where(fine, 1.0 / jnp.where(fine, pivot, 1.0), 0.0)

    i0 = inverse_of(h00, 0.0 * h00)
    l1, l2 = h01 * i0, h02 * i0
    i1 = inverse_of(h11 - l1 * h01, h11)
    e = h12 - l1 * h02
    l3 = e * i1
    i2 = inverse_of(h22 - l2 * h02 - l3 * e, h22)
    z1 = m01 - l1 * m00
    z2 = m11 - l2 * m00 - l3 * z1
    y2 = z2 * i2
    y1 = z1 * i1 - l3 * y2
    y0 = m00 * i0 - l1 * y1 - l2 * y2
    return y0 * ia, y1 * ia, y2 * ia


def second_kernel(*refs):
    arrived, v0, v1, v2, other = refs[:5]
    ghosts, inv_alpha, vector, outputs = refs[5:17], refs[17], refs[18], refs[19:]
    y0, y1, y2 = weights_of(arrived, inv_alpha[0])
    keep = lax.broadcasted_iota(jnp.int32, (ROWS, 1), 0) < ROWS - 1

    def start(explicit, a, b, c):
        weight = explicit[ROWS - 1 :]
        return jnp.where(keep, explicit, 0.0) + weight * (y0 * a + y1 * b + y2 * c)

    vector[...] = start(other[...], v0[...], v1[...], v2[...])
    for c in range(4):
        both = ghosts[c]
        outputs[c][...] = start(
            both[ROWS:, :], both[:ROWS, :], ghosts[4 + c][...], ghosts[8 + c][...]
        )


def last_kernel(arrived, v0, v1, v2, n0, n1, n2, inv_alpha, member, trace, interior):
    y0, y1, y2 = weights_of(arrived, inv_alpha[0])
    interior[...] = y0 * n0[...] + y1 * n1[...] + y2 * n2[...]

    @pl.when(pl.program_id(0) == 0)
    def _():
        nodes, owned = trace.shape
        mine = pl.ds(pl.multiple_of(member[0] * owned, LANES), owned)
        trace[...] = (y0 * v0[:, mine] + y1 * v1[:, mine] + y2 * v2[:, mine])[:nodes]


def body(
    source_one,
    source_two,
    face_mass,
    penalty,
    interior_scale,
    coupling,
    inverse_block,
    element_faces,
    element_type,
    send_faces,
):
    members = lax.axis_size("sub")
    nodes, owned = source_one.shape
    group_width = members * owned
    elements = element_faces.shape[1]
    unknowns = coupling.shape[0]
    padded = -(-unknowns // LANES) * LANES
    reach = lax.axis_size(DOM) // 4
    domains = lax.axis_size(DOM)
    odd = lax.axis_index("core") % 2 == 1
    odd_far = lax.axis_index("zq") % 2 == 1

    pairs = (
        [(i, i + 1 if i % 2 == 0 else i - 1) for i in range(domains)],
        [(i, (i + 1 if i % 2 == 1 else i - 1) % domains) for i in range(domains)],
        [
            (i, (i + reach if (i // reach) % 2 == 0 else i - reach) % domains)
            for i in range(domains)
        ],
        [
            (i, (i + reach if (i // reach) % 2 == 1 else i - reach) % domains)
            for i in range(domains)
        ],
    )

    def exchange(payload):
        got = []
        for c in range(4):
            got.append(lax.ppermute(payload[c], DOM, pairs[c]))
        return got

    to_send = jnp.concatenate(
        [
            jnp.where(odd, send_faces[1], send_faces[0]),
            jnp.where(odd, send_faces[0], send_faces[1]),
            jnp.where(odd_far, send_faces[3], send_faces[2]),
            jnp.where(odd_far, send_faces[2], send_faces[3]),
        ]
    )
    near = element_faces - group_width
    direction = near // LANES
    swapped = jnp.where(direction < 2, jnp.where(odd, 0, 1), jnp.where(odd_far, 0, 1))
    remote = element_faces + LANES * jnp.where(
        swapped == 1, jnp.where(direction % 2 == 0, 1, -1), 0
    )
    faces = jnp.where(element_faces < group_width, element_faces, remote)
    faces = faces.reshape(1, -1)
    slots = faces.shape[1]
    spread = jnp.broadcast_to(faces.reshape(slots, 1), (slots, LANES))
    send_list = to_send.reshape(1, -1)
    send_spread = jnp.broadcast_to(to_send[:, None], (to_send.shape[0], LANES))
    mask = 1.0 - (element_type == 1).astype(F32)[None, :]
    weight = penalty[None, :]

    by_slot = coupling.reshape(unknowns, nodes, 6).transpose(0, 2, 1)
    by_slot = jnp.pad(by_slot, ((0, padded - unknowns), (0, 0), (0, ROWS - nodes)))
    by_slot = by_slot.reshape(padded, 6 * ROWS)
    extra = padded - unknowns
    padded_inverse = jnp.pad(inverse_block, ((0, extra), (0, extra)))
    lift, by_slot, inverse = (
        rounded_halves(m) for m in (by_slot.T, by_slot, padded_inverse)
    )
    scale = jnp.pad(interior_scale, ((0, extra), (0, 0)))

    spectrum = jnp.sum(coupling * jnp.dot(inverse_block, coupling)) / coupling.shape[1]
    inv_alpha = (1.0 / (0.6 + 2.4 * (1.1 + 1.35 * spectrum))).reshape(1)

    tile = shape(ROWS, LANES)
    mine = kernel_call(
        start_kernel,
        shape(members, 2 * ROWS, owned),
        source_one,
        source_two,
        face_mass[None, :],
        specs=[COPIED] * 3,
    )
    everyone = lax.all_to_all(mine, "sub", 0, 0, tiled=True)
    v0, other, *outgoing = kernel_call(
        first_kernel,
        (shape(ROWS, group_width), shape(ROWS, group_width)) + (shape(2 * ROWS, LANES),) * 4,
        everyone,
        send_list,
        inv_alpha,
        specs=[VMEM, VMEM, SMEM],
    )
    start_ghosts = exchange(outgoing)
    member = lax.axis_index("sub").astype(jnp.int32).reshape(1)
    scratch = [pltpu.VMEM((6 * ROWS, elements), F32)]
    copies = [pltpu.VMEM((padded, elements), F32), pltpu.SemaphoreType.DMA]

    def apply(vector, ghosts, keep_inner):
        inner_shape = (shape(padded, elements),) if keep_inner else ()
        outs = kernel_call(
            apply_kernel,
            (tile,) * 4 + (shape(3 * ROWS, slots, dtype=BF16),) + inner_shape,
            vector,
            *ghosts,
            faces,
            spread,
            mask,
            weight,
            *by_slot,
            *lift,
            *inverse,
            scale,
            specs=[VMEM] + [COPIED if ghosts[0].shape[0] > ROWS else VMEM] * 4 + [VMEM] * 11,
            out_specs=(VMEM,) * 5 + ((ANY,) if keep_inner else ()),
            scratch=scratch + (copies if keep_inner else []),
        )
        returned, pieces, inner = outs[:4], outs[4], outs[5:]
        back = exchange(returned)
        placed = kernel_call(place_kernel, shape(ROWS, group_width), pieces, spread)
        packed = kernel_call(
            pack_kernel,
            shape(members, 24 * (group_width // LANES) + 24, LANES),
            placed,
            *back,
            send_spread,
        )
        arrived = lax.all_to_all(packed, "sub", 0, 0, tiled=True)
        following, *outgoing = kernel_call(
            next_kernel,
            (shape(ROWS, group_width),) + (tile,) * 4,
            arrived,
            vector,
            other,
            send_list,
            inv_alpha,
            specs=[VMEM] * 4 + [SMEM],
        )
        return following, exchange(outgoing), list(inner)

    count = 1
    for axis in NEAR:
        count *= lax.axis_size(axis)
    far = domains * members // count

    def section(v0, g0, keep_inner):
        inner_shape = (shape(padded, elements),) if keep_inner else ()
        v1, g1, n0 = apply(v0, g0, keep_inner)
        v2, g2, n1 = apply(v1, g1, keep_inner)
        face_part = kernel_call(
            moment_kernel, shape(8, LANES), v0, v1, v2, other, inv_alpha, specs=[VMEM] * 4 + [SMEM]
        )
        moments, *n2 = kernel_call(
            energy_kernel,
            (shape(count, 8, LANES),) + inner_shape,
            v2,
            *g2,
            faces,
            mask,
            weight,
            *by_slot,
            *inverse,
            scale,
            face_part,
            inv_alpha,
            specs=[VMEM] * 14 + [SMEM],
            scratch=scratch,
        )
        arrived = lax.all_to_all(moments, NEAR, 0, 0, tiled=True)
        moments = kernel_call(sum_kernel, shape(far, 8, LANES), arrived)
        arrived = lax.all_to_all(moments, FAR, 0, 0, tiled=True)
        return (v0, v1, v2), g1 + g2, n0 + n1 + n2, arrived

    vs, later_ghosts, _, arrived = section(v0, start_ghosts, False)
    u0, *h0 = kernel_call(
        second_kernel,
        (shape(ROWS, group_width),) + (tile,) * 4,
        arrived,
        *vs,
        other,
        *start_ghosts,
        *later_ghosts,
        inv_alpha,
        specs=[VMEM] * 17 + [SMEM],
    )
    vs, _, inners, arrived = section(u0, h0, True)
    rows = pl.BlockSpec((LANES, elements), lambda i: (i, 0))
    return pl.pallas_call(
        last_kernel,
        out_shape=(shape(nodes, owned), shape(unknowns, elements)),
        grid=(padded // LANES,),
        in_specs=[VMEM] * 4 + [rows] * 3 + [SMEM] * 2,
        out_specs=(pl.BlockSpec((nodes, owned), lambda i: (0, 0)), rows),
        name="last",
        compiler_params=pltpu.CompilerParams(vmem_limit_bytes=16 << 20),
    )(arrived, *vs, *inners, inv_alpha, member)


def solution(mesh):
    sub = mesh.shape["sub"]
    split = Mesh(mesh.devices.reshape(4, 4, 4, 2, sub), ALL)
    return jax.shard_map(
        body,
        mesh=split,
        in_specs=(
            P(None, ALL),
            P(None, ALL),
            P(ALL),
            P(ALL),
            P(None, ALL),
            P(),
            P(),
            P(None, ALL),
            P(ALL),
            P(None, ALL),
        ),
        out_specs=(P(None, ALL), P(None, ALL)),
        check_vma=False,
    )
```

```python
import jax
import jax.numpy as jnp
from jax import lax
from jax.experimental import pallas as pl
from jax.experimental.pallas import tpu as pltpu
from jax.sharding import Mesh
from jax.sharding import PartitionSpec as P

F32 = jnp.float32
BF16 = jnp.bfloat16
LANES = 128
ROWS = 32
DOM = ("zq", "zr", "x", "core")
ALL = ("zq", "zr", "x", "core", "sub")
NEAR = ("x", "core", "sub")
FAR = ("zq", "zr")
VMEM = pl.BlockSpec(memory_space=pltpu.VMEM)
ANY = pl.BlockSpec(memory_space=pl.ANY)
COPIED = pl.BlockSpec()
SMEM = pl.BlockSpec(memory_space=pltpu.SMEM)


def kernel_call(body, outs, *args, specs=None, out_specs=None, scratch=()):
    return pl.pallas_call(
        body,
        out_shape=outs,
        in_specs=specs or [VMEM] * len(args),
        out_specs=out_specs or jax.tree.map(lambda _: VMEM, outs),
        scratch_shapes=scratch,
        compiler_params=pltpu.CompilerParams(vmem_limit_bytes=32 << 20),
    )(*args)


def shape(*dims, dtype=F32):
    return jax.ShapeDtypeStruct(dims, dtype)


def split3(x):
    high = x.astype(BF16)
    rest = x - high.astype(F32)
    middle = rest.astype(BF16)
    low = (rest - middle.astype(F32)).astype(BF16)
    return jnp.concatenate([high, middle, low], axis=0)


def join3(y):
    return y[:ROWS] + y[ROWS : 2 * ROWS] + y[2 * ROWS :]


def halves(x):
    high = x.astype(BF16)
    return high, (x - high.astype(F32)).astype(BF16)


def rounded_halves(x):
    high = lax.reduce_precision(x, exponent_bits=8, mantissa_bits=7)
    return high.astype(BF16), (x - high).astype(BF16)


def product(left, right):
    high, low = halves(right)
    return jnp.dot(left[0][...], high, preferred_element_type=F32) + (
        jnp.dot(left[0][...], low, preferred_element_type=F32)
        + jnp.dot(left[1][...], high, preferred_element_type=F32)
    )


def pick_lanes(index, tiles, groups):
    index = jnp.broadcast_to(index, (8, LANES))
    block = lax.shift_right_logical(index, 7)
    lane = jnp.bitwise_and(index, LANES - 1)
    count, load = tiles
    picked = [jnp.zeros((8, LANES), F32) for _ in range(groups)]
    for source in range(count):
        here = block == source
        for group in range(groups):
            moved = jnp.take_along_axis(load(source, group), lane, axis=1)
            picked[group] = jnp.where(here, moved, picked[group])
    return picked


def place_lanes(pieces, spread, first, width):
    offset = spread - lax.broadcasted_iota(jnp.int32, spread.shape, 1)
    hits = [(offset == (first + k)).astype(F32).astype(BF16) for k in range(0, width, LANES)]
    return join3(jnp.dot(pieces, jnp.concatenate(hits, axis=1), preferred_element_type=F32))


def lane_sums(x):
    total = x[:, :LANES]
    for begin in range(LANES, x.shape[1], LANES):
        total = total + x[:, begin : begin + LANES]
    return jnp.sum(total, axis=0, keepdims=True)


def start_kernel(one, two, mass, outgoing, near_one, near_two, near_mass, ready):
    copies = [
        pltpu.make_async_copy(source, target, ready.at[k])
        for k, (source, target) in enumerate(
            ((one, near_one), (two, near_two), (mass, near_mass))
        )
    ]
    for copy in copies:
        copy.start()
    nodes, owned = one.shape
    for member in range(outgoing.shape[0]):
        outgoing[member, nodes:ROWS, :] = jnp.zeros((ROWS - nodes, owned), F32)
        outgoing[member, ROWS + nodes : 2 * ROWS - 1, :] = jnp.zeros((ROWS - 1 - nodes, owned), F32)
    for copy in copies:
        copy.wait()
    for member in range(outgoing.shape[0]):
        outgoing[member, :nodes, :] = near_one[...]
        outgoing[member, ROWS : ROWS + nodes, :] = near_two[...]
        outgoing[member, 2 * ROWS - 1 :, :] = near_mass[...].reshape(1, owned)


def first_kernel(arrived, send_list, *refs):
    v0, other, *outgoing = refs[-6:]
    blocks = arrived.shape[2] // LANES
    for member in range(arrived.shape[0]):
        for block in range(blocks):
            to = pl.ds((member * blocks + block) * LANES, LANES)
            v0[:, to] = arrived[member, :ROWS, pl.ds(block * LANES, LANES)]
            other[:, to] = arrived[member, ROWS:, pl.ds(block * LANES, LANES)]

    def load(source, group):
        member, block = divmod(source, blocks)
        return arrived[member, pl.ds(group * 8, 8), pl.ds(block * LANES, LANES)]

    for channel in range(4):
        index = send_list[:, pl.ds(channel * LANES, LANES)]
        picked = pick_lanes(index, (arrived.shape[0] * blocks, load), 2 * ROWS // 8)
        for group, tile in enumerate(picked):
            outgoing[channel][pl.ds(group * 8, 8), :] = tile


def gather_slots(vector, ghosts, faces, mask, weighted):
    count = vector.shape[1] // LANES
    width = mask.shape[1]
    near = vector[...]
    pieces = split3(jnp.concatenate([near] + [g[:ROWS, :] for g in ghosts], axis=1))

    def load(source, group):
        if source < count:
            return vector[pl.ds(group * 8, 8), pl.ds(source * LANES, LANES)]
        return ghosts[source - count][pl.ds(group * 8, 8), :]

    def step(slot, carry):
        other = slot + 3
        index = faces[:, pl.ds(pl.multiple_of(other * width, LANES), width)]
        lines = lax.broadcasted_iota(jnp.int32, (pieces.shape[1], width), 0)
        hits = (lines == index).astype(F32).astype(BF16)
        values = join3(jnp.dot(pieces, hits, preferred_element_type=F32))
        for block in range(width // LANES):
            begin = pl.multiple_of(slot * width + block * LANES, LANES)
            picked = pick_lanes(faces[:, pl.ds(begin, LANES)], (count + 4, load), ROWS // 8)
            for group, tile in enumerate(picked):
                row = pl.multiple_of(slot * ROWS + group * 8, 8)
                weighted[pl.ds(row, 8), pl.ds(block * LANES, LANES)] = tile
        weighted[pl.ds(pl.multiple_of(other * ROWS, ROWS), ROWS), :] = values
        return carry

    lax.fori_loop(0, 3, step, 0)
    weighted[pl.ds(5 * ROWS, ROWS), :] = weighted[pl.ds(5 * ROWS, ROWS), :] * mask[...]


def apply_kernel(*refs):
    vector, *ghosts = refs[:5]
    faces, spread, mask, penalty = refs[5:9]
    coupling, lift, inverse = refs[9:11], refs[11:13], refs[13:15]
    scale = refs[15]
    returned, pieces = refs[16:20], refs[20]
    keep = len(refs) > 22
    weighted = refs[22] if keep else refs[21]
    gather_slots(vector, ghosts, faces, mask, weighted)
    w = weighted[...]
    s = scale[...]
    coupled = s * product(coupling, w)
    inside = s * product(inverse, coupled)
    if keep:
        refs[23][...] = inside
        leaving = pltpu.make_async_copy(refs[23], refs[21], refs[24])
        leaving.start()
    contrib = penalty[...] * w + product(lift, inside)
    slots = [contrib[k * ROWS : (k + 1) * ROWS] for k in range(6)]
    slots[5] = slots[5] * mask[...]
    parts = split3(jnp.concatenate(slots, axis=1))
    pieces[...] = parts
    width = 5 * mask.shape[1]
    for pair in range(2):
        onto = place_lanes(
            parts[:, :width], spread[:width], vector.shape[1] + pair * 2 * LANES, 2 * LANES
        )
        returned[2 * pair][...] = onto[:, :LANES]
        returned[2 * pair + 1][...] = onto[:, LANES:]
    if keep:
        leaving.wait()


def place_kernel(pieces, spread, placed):
    for begin in range(0, placed.shape[1], 2 * LANES):
        placed[:, pl.ds(begin, 2 * LANES)] = place_lanes(
            pieces[...], spread[...], begin, 2 * LANES
        )


def pack_kernel(placed, r0, r1, r2, r3, spread, packed):
    blocks = placed.shape[1] // LANES
    parts = split3(jnp.concatenate([r[...] for r in (r0, r1, r2, r3)], axis=1))
    packed[:, pl.ds(24 * blocks, 24), :] = jnp.zeros((4, 24, LANES), F32)
    for begin in range(0, blocks, 2):
        onto = place_lanes(parts, spread[...], begin * LANES, 2 * LANES)
        onto = onto + placed[:, pl.ds(begin * LANES, 2 * LANES)]
        for k in range(2):
            block = begin + k
            half = onto[:, k * LANES : (k + 1) * LANES]
            for member in range(4):
                for group in range(3):
                    packed[member, pl.ds((group * blocks + block) * 8, 8), :] = half[
                        group * 8 : group * 8 + 8
                    ]
                packed[member, pl.ds(24 * blocks + block, 1), :] = half[24:25]


def next_kernel(arrived, before, other, send_list, inv_alpha, vector, *outgoing):
    blocks = before.shape[1] // LANES
    ia = inv_alpha[0]

    def total(begin, size):
        rows = pl.ds(begin, size)
        return (arrived[0, rows, :] + arrived[1, rows, :]) + (
            arrived[2, rows, :] + arrived[3, rows, :]
        )

    vector[pl.ds(24, 8), :] = jnp.zeros((8, vector.shape[1]), F32)
    for block in range(blocks):
        lanes = pl.ds(block * LANES, LANES)
        weight = other[pl.ds(ROWS - 1, 1), lanes]
        for group in range(3):
            old = before[pl.ds(group * 8, 8), lanes]
            new = (weight * old + total((group * blocks + block) * 8, 8)) * ia - old
            vector[pl.ds(group * 8, 8), lanes] = new
        old = before[pl.ds(24, 1), lanes]
        new = (weight * old + total(24 * blocks + block, 1)) * ia - old
        vector[pl.ds(24, 1), lanes] = new

    def load(source, group):
        return vector[pl.ds(group * 8, 8), pl.ds(source * LANES, LANES)]

    for channel in range(4):
        index = send_list[:, pl.ds(channel * LANES, LANES)]
        for group, tile in enumerate(pick_lanes(index, (blocks, load), ROWS // 8)):
            outgoing[channel][pl.ds(group * 8, 8), :] = tile


def moment_kernel(v0, v1, v2, other, inv_alpha, moments):
    a, b, c = v0[...], v1[...], v2[...]
    weight = other[pl.ds(ROWS - 1, 1), :] * inv_alpha[0]
    group = [lane_sums(p) for p in (a * a, a * b, b * b, b * c, c * c, weight * (c * c))]
    moments[...] = 0.25 * jnp.concatenate(group + [jnp.zeros((2, LANES), F32)], axis=0)


def energy_kernel(*refs):
    vector, *ghosts = refs[:5]
    faces, mask, penalty = refs[5:8]
    coupling, inverse = refs[8:10], refs[10:12]
    scale, face_part, inv_alpha, moments = refs[12:16]
    weighted = refs[-1]
    gather_slots(vector, ghosts, faces, mask, weighted)
    w = weighted[...]
    s = scale[...]
    coupled = s * product(coupling, w)
    inside = product(inverse, coupled)
    if len(refs) == 18:
        refs[16][...] = s * inside
    local = lane_sums(coupled * inside) + lane_sums(penalty[...] * (w * w))
    row = lax.broadcasted_iota(jnp.int32, (8, LANES), 0)
    tile = face_part[...] + jnp.where(row == 5, local * inv_alpha[0], 0.0)
    for k in range(moments.shape[0]):
        moments[k] = tile


def sum_kernel(arrived, moments):
    total = arrived[0]
    for k in range(1, arrived.shape[0]):
        total = total + arrived[k]
    for k in range(moments.shape[0]):
        moments[k] = total


def weights_of(arrived, ia):
    total = arrived[0]
    for k in range(1, arrived.shape[0]):
        total = total + arrived[k]
    m = jnp.sum(total, axis=1, keepdims=True)
    m00, m01, m11, m12, m22, energy = (m[k : k + 1] for k in range(6))
    h00, h01, h02 = m00 + m01, m01 + m11, m11 + m12
    h11, h12, h22 = m11 + m12, m12 + m22, energy

    def inverse_of(pivot, whole):
        fine = pivot > 1e-7 * whole
        return jnp.where(fine, 1.0 / jnp.where(fine, pivot, 1.0), 0.0)

    i0 = inverse_of(h00, 0.0 * h00)
    l1, l2 = h01 * i0, h02 * i0
    i1 = inverse_of(h11 - l1 * h01, h11)
    e = h12 - l1 * h02
    l3 = e * i1
    i2 = inverse_of(h22 - l2 * h02 - l3 * e, h22)
    z1 = m01 - l1 * m00
    z2 = m11 - l2 * m00 - l3 * z1
    y2 = z2 * i2
    y1 = z1 * i1 - l3 * y2
    y0 = m00 * i0 - l1 * y1 - l2 * y2
    return y0 * ia, y1 * ia, y2 * ia


def second_kernel(*refs):
    arrived, v0, v1, v2, other = refs[:5]
    ghosts, inv_alpha, vector, outputs = refs[5:17], refs[17], refs[18], refs[19:]
    y0, y1, y2 = weights_of(arrived, inv_alpha[0])
    keep = lax.broadcasted_iota(jnp.int32, (ROWS, 1), 0) < ROWS - 1

    def start(explicit, a, b, c):
        weight = explicit[ROWS - 1 :]
        return jnp.where(keep, explicit, 0.0) + weight * (y0 * a + y1 * b + y2 * c)

    vector[...] = start(other[...], v0[...], v1[...], v2[...])
    for c in range(4):
        both = ghosts[c]
        outputs[c][...] = start(
            both[ROWS:, :], both[:ROWS, :], ghosts[4 + c][...], ghosts[8 + c][...]
        )


def last_kernel(arrived, v0, v1, v2, inv_alpha, member, trace, weights):
    y0, y1, y2 = weights_of(arrived, inv_alpha[0])
    nodes, owned = trace.shape
    mine = pl.ds(pl.multiple_of(member[0] * owned, LANES), owned)
    trace[...] = (y0 * v0[:, mine] + y1 * v1[:, mine] + y2 * v2[:, mine])[:nodes]
    for k, y in enumerate((y0, y1, y2)):
        weights[k : k + 1, :] = jnp.broadcast_to(y, (1, weights.shape[1]))


def body(
    source_one,
    source_two,
    face_mass,
    penalty,
    interior_scale,
    coupling,
    inverse_block,
    element_faces,
    element_type,
    send_faces,
):
    members = lax.axis_size("sub")
    nodes, owned = source_one.shape
    group_width = members * owned
    elements = element_faces.shape[1]
    unknowns = coupling.shape[0]
    padded = -(-unknowns // LANES) * LANES
    reach = lax.axis_size(DOM) // 4
    domains = lax.axis_size(DOM)
    odd = lax.axis_index("core") % 2 == 1
    odd_far = lax.axis_index("zq") % 2 == 1

    pairs = (
        [(i, i + 1 if i % 2 == 0 else i - 1) for i in range(domains)],
        [(i, (i + 1 if i % 2 == 1 else i - 1) % domains) for i in range(domains)],
        [
            (i, (i + reach if (i // reach) % 2 == 0 else i - reach) % domains)
            for i in range(domains)
        ],
        [
            (i, (i + reach if (i // reach) % 2 == 1 else i - reach) % domains)
            for i in range(domains)
        ],
    )

    def exchange(payload):
        got = []
        for c in range(4):
            got.append(lax.ppermute(payload[c], DOM, pairs[c]))
        return got

    to_send = jnp.concatenate(
        [
            jnp.where(odd, send_faces[1], send_faces[0]),
            jnp.where(odd, send_faces[0], send_faces[1]),
            jnp.where(odd_far, send_faces[3], send_faces[2]),
            jnp.where(odd_far, send_faces[2], send_faces[3]),
        ]
    )
    near = element_faces - group_width
    direction = near // LANES
    swapped = jnp.where(direction < 2, jnp.where(odd, 0, 1), jnp.where(odd_far, 0, 1))
    remote = element_faces + LANES * jnp.where(
        swapped == 1, jnp.where(direction % 2 == 0, 1, -1), 0
    )
    faces = jnp.where(element_faces < group_width, element_faces, remote)
    faces = faces.reshape(1, -1)
    slots = faces.shape[1]
    spread = jnp.broadcast_to(faces.reshape(slots, 1), (slots, LANES))
    send_list = to_send.reshape(1, -1)
    send_spread = jnp.broadcast_to(to_send[:, None], (to_send.shape[0], LANES))
    mask = 1.0 - (element_type == 1).astype(F32)[None, :]
    weight = penalty[None, :]

    by_slot = coupling.reshape(unknowns, nodes, 6).transpose(0, 2, 1)
    by_slot = jnp.pad(by_slot, ((0, padded - unknowns), (0, 0), (0, ROWS - nodes)))
    by_slot = by_slot.reshape(padded, 6 * ROWS)
    extra = padded - unknowns
    padded_inverse = jnp.pad(inverse_block, ((0, extra), (0, extra)))
    lift, by_slot, inverse = (
        rounded_halves(m) for m in (by_slot.T, by_slot, padded_inverse)
    )
    scale = jnp.pad(interior_scale, ((0, extra), (0, 0)))

    spectrum = jnp.sum(coupling * jnp.dot(inverse_block, coupling)) / coupling.shape[1]
    inv_alpha = (1.0 / (0.6 + 2.4 * (1.1 + 1.35 * spectrum))).reshape(1)

    tile = shape(ROWS, LANES)
    mine = kernel_call(
        start_kernel,
        shape(members, 2 * ROWS, owned),
        source_one,
        source_two,
        face_mass,
        specs=[ANY] * 3,
        scratch=[
            pltpu.VMEM((nodes, owned), F32),
            pltpu.VMEM((nodes, owned), F32),
            pltpu.VMEM((owned,), F32),
            pltpu.SemaphoreType.DMA((3,)),
        ],
    )
    early = (inv_alpha, *by_slot, *lift, *inverse, scale, spread, send_spread, mask, faces)
    everyone = lax.all_to_all(mine, "sub", 0, 0, tiled=True)
    v0, other, *outgoing = kernel_call(
        first_kernel,
        (shape(ROWS, group_width), shape(ROWS, group_width)) + (shape(2 * ROWS, LANES),) * 4,
        everyone,
        send_list,
        *early,
        specs=[VMEM, VMEM] + [ANY] * len(early),
    )
    start_ghosts = exchange(outgoing)
    member = lax.axis_index("sub").astype(jnp.int32).reshape(1)
    scratch = [pltpu.VMEM((6 * ROWS, elements), F32)]
    copies = [pltpu.VMEM((padded, elements), F32), pltpu.SemaphoreType.DMA]

    def apply(vector, ghosts, keep_inner):
        inner_shape = (shape(padded, elements),) if keep_inner else ()
        outs = kernel_call(
            apply_kernel,
            (tile,) * 4 + (shape(3 * ROWS, slots, dtype=BF16),) + inner_shape,
            vector,
            *ghosts,
            faces,
            spread,
            mask,
            weight,
            *by_slot,
            *lift,
            *inverse,
            scale,
            specs=[VMEM] + [COPIED if ghosts[0].shape[0] > ROWS else VMEM] * 4 + [VMEM] * 11,
            out_specs=(VMEM,) * 5 + ((ANY,) if keep_inner else ()),
            scratch=scratch + (copies if keep_inner else []),
        )
        returned, pieces, inner = outs[:4], outs[4], outs[5:]
        back = exchange(returned)
        placed = kernel_call(place_kernel, shape(ROWS, group_width), pieces, spread)
        packed = kernel_call(
            pack_kernel,
            shape(members, 24 * (group_width // LANES) + 24, LANES),
            placed,
            *back,
            send_spread,
        )
        arrived = lax.all_to_all(packed, "sub", 0, 0, tiled=True)
        following, *outgoing = kernel_call(
            next_kernel,
            (shape(ROWS, group_width),) + (tile,) * 4,
            arrived,
            vector,
            other,
            send_list,
            inv_alpha,
            specs=[VMEM] * 4 + [SMEM],
        )
        return following, exchange(outgoing), list(inner)

    count = 1
    for axis in NEAR:
        count *= lax.axis_size(axis)
    far = domains * members // count

    def section(v0, g0, keep_inner):
        inner_shape = (shape(padded, elements),) if keep_inner else ()
        v1, g1, n0 = apply(v0, g0, keep_inner)
        v2, g2, n1 = apply(v1, g1, keep_inner)
        face_part = kernel_call(
            moment_kernel, shape(8, LANES), v0, v1, v2, other, inv_alpha, specs=[VMEM] * 4 + [SMEM]
        )
        moments, *n2 = kernel_call(
            energy_kernel,
            (shape(count, 8, LANES),) + inner_shape,
            v2,
            *g2,
            faces,
            mask,
            weight,
            *by_slot,
            *inverse,
            scale,
            face_part,
            inv_alpha,
            specs=[VMEM] * 14 + [SMEM],
            scratch=scratch,
        )
        arrived = lax.all_to_all(moments, NEAR, 0, 0, tiled=True)
        moments = kernel_call(sum_kernel, shape(far, 8, LANES), arrived)
        arrived = lax.all_to_all(moments, FAR, 0, 0, tiled=True)
        return (v0, v1, v2), g1 + g2, n0 + n1 + n2, arrived

    vs, later_ghosts, _, arrived = section(v0, start_ghosts, False)
    u0, *h0 = kernel_call(
        second_kernel,
        (shape(ROWS, group_width),) + (tile,) * 4,
        arrived,
        *vs,
        other,
        *start_ghosts,
        *later_ghosts,
        inv_alpha,
        specs=[VMEM] * 17 + [SMEM],
    )
    vs, _, inners, arrived = section(u0, h0, True)
    trace_two, weights = kernel_call(
        last_kernel,
        (shape(nodes, owned), shape(3, elements)),
        arrived,
        *vs,
        inv_alpha,
        member,
        specs=[VMEM] * 4 + [SMEM] * 2,
    )
    interior = sum(weights[k][None, :] * inners[k][:unknowns] for k in range(3))
    return trace_two, interior


def solution(mesh):
    sub = mesh.shape["sub"]
    split = Mesh(mesh.devices.reshape(4, 4, 4, 2, sub), ALL)
    return jax.shard_map(
        body,
        mesh=split,
        in_specs=(
            P(None, ALL),
            P(None, ALL),
            P(ALL),
            P(ALL),
            P(None, ALL),
            P(),
            P(),
            P(None, ALL),
            P(ALL),
            P(None, ALL),
        ),
        out_specs=(P(None, ALL), P(None, ALL)),
        check_vma=False,
    )
```
